32 devices in a mesh: dp: 4 (over z), sx: 4 (over y, core), sy: 2 (over x).
Axes of the slice: x: 2, y: 2, z: 4, core: 2. Of those that a mesh axis runs over, the one named last changes fastest.
Arguments:
- volume: bfloat16 [4, 4, 16, 16, 128], P('dp', None, 'sx', 'sy'), may hold values from -6 to 6
- first_weight: bfloat16 [32, 108], replicated, may hold values from -0.625 to 0.625
- second_weight: bfloat16 [64, 864], replicated, may hold values from -0.21875 to 0.21875
- cotangent: bfloat16 [4, 64, 8, 8, 64], P('dp', None, 'sx', 'sy'), may hold values from -6 to 6
Outputs:
- grad_first: float32 [32, 108], replicated
- grad_second: float32 [64, 864], replicated
The draws below stay inside these ranges and needn't reach their ends.
All inputs are finite; a program needn't handle non-finite values.
Results may differ from the reference program's by a relative error of at most 0.014.
Values may be sent and summed in bfloat16 or wider, within the bound.
No kernel may reach another device: no remote copies, remote signals or barrier semaphores. Data moves between devices by JAX's collectives and lax.ppermute only.
A program may use at most 64 MiB of HBM per device.

```python
import jax
import jax.numpy as jnp
from jax import lax

C_IN = 4
C1 = 32
C2 = 64
CZ = 128
BATCH = 4
NX = 16
NY = 16


def shard_levels(rng, extent, cuts, least, largest):
    factor_of = 1.0
    for axis_at, shards_of in cuts:
        heights = jax.random.uniform(jax.random.fold_in(jax.random.fold_in(rng, 6), axis_at), (shards_of,), jnp.float32, least / len(cuts), largest / len(cuts))
        factor_of = factor_of * jnp.repeat(jnp.exp(heights), extent[axis_at] // shards_of).reshape((-1,) + (1,) * (len(extent) - 1 - axis_at))
    return factor_of


def bell_draw(rng, dims, width, limit, split=(), dtype=jnp.bfloat16):
    values = width * jax.random.normal(rng, dims, jnp.float32)
    if split:
        values = values * shard_levels(rng, dims, split, -0.22, 0.18)
    return jnp.clip(values, -limit, limit).astype(dtype)


def setup_inputs(seed: int = 0) -> dict:
    streams_of = jax.random.split(jax.random.key(seed), 5)
    volume = bell_draw(streams_of[0], (BATCH, C_IN, NX, NY, CZ), 1.0, 6.0, ((0, 4), (2, 4), (3, 2)))
    first_weight = bell_draw(streams_of[1], (C1, 27 * C_IN), (27 * C_IN) ** -0.5, 0.625)
    second_weight = bell_draw(streams_of[2], (C2, 27 * C1), (27 * C1) ** -0.5, 0.21875)
    cotangent = bell_draw(streams_of[3], (BATCH, C2, NX // 2, NY // 2, CZ // 2), 1.0, 6.0, ((0, 4), (2, 4), (3, 2)))
    return dict(volume=volume, first_weight=first_weight, second_weight=second_weight, cotangent=cotangent)


def leaky(value):
    return 0.3 * value + 0.7 * jax.nn.softplus(value)

def slope(value):
    return 0.3 + 0.7 * jax.nn.sigmoid(value)

def patches(padded, width_x, width_y, width_z):
    columns = []
    for shift_x in range(3):
        for shift_y in range(3):
            for shift_z in range(3):
                columns.append(padded[:, shift_x:shift_x + width_x, shift_y:shift_y + width_y, shift_z:shift_z + width_z])
    stacked = jnp.concatenate(columns, 0)
    return stacked.reshape(stacked.shape[0], width_x * width_y * width_z)

def pad_all(field):
    return jnp.pad(field, ((0, 0), (1, 1), (1, 1), (1, 1)))

def one_sample(first_weight, second_weight, sample, cot):
    chans, width_x, width_y, width_z = sample.shape
    fine_cols = patches(pad_all(sample), width_x, width_y, width_z)
    pre_first = jnp.dot(first_weight, fine_cols, preferred_element_type=jnp.float32)
    hidden = leaky(pre_first).astype(jnp.bfloat16)
    inner = hidden.shape[0]
    half_x, half_y, half_z = (width_x // 2, width_y // 2, width_z // 2)
    pooled = (hidden.astype(jnp.float32).reshape(inner, half_x, 2, half_y, 2, half_z, 2).sum(axis=(2, 4, 6)) * 0.125).astype(jnp.bfloat16)
    coarse_cols = patches(pad_all(pooled), half_x, half_y, half_z)
    pre_second = jnp.dot(second_weight, coarse_cols, preferred_element_type=jnp.float32)
    outer = pre_second.shape[0]
    back = (cot.reshape(outer, -1).astype(jnp.float32) * slope(pre_second)).astype(jnp.bfloat16)
    second_part = lax.dot_general(back, coarse_cols, (((1,), (1,)), ((), ())), preferred_element_type=jnp.float32)
    back_cols = patches(pad_all(back.reshape(outer, half_x, half_y, half_z)), half_x, half_y, half_z)
    mirrored = second_weight.reshape(outer, 27, inner)[:, ::-1, :].transpose(2, 1, 0).reshape(inner, 27 * outer)
    up = jnp.dot(mirrored, back_cols, preferred_element_type=jnp.float32)
    spread = jnp.broadcast_to(up.reshape(inner, half_x, 1, half_y, 1, half_z, 1), (inner, half_x, 2, half_y, 2, half_z, 2)).reshape(inner, -1)
    lower = (spread * 0.125 * slope(pre_first)).astype(jnp.bfloat16)
    first_part = lax.dot_general(lower, fine_cols, (((1,), (1,)), ((), ())), preferred_element_type=jnp.float32)
    return (first_part, second_part)

def reference(volume, first_weight, second_weight, cotangent):

    def step(pair):
        return one_sample(first_weight, second_weight, pair[0], pair[1])
    firsts, seconds = lax.map(step, (volume, cotangent))
    coarse_count = volume.shape[0] * volume.shape[2] * volume.shape[3] * volume.shape[4] // 8
    scale_second = 1.0 / jnp.sqrt(jnp.float32(coarse_count))
    scale_first = 1.0 / jnp.sqrt(jnp.float32(coarse_count * 8))
    return (lax.optimization_barrier(jnp.sum(firsts, 0)) * scale_first, lax.optimization_barrier(jnp.sum(seconds, 0)) * scale_second)
```

```python
import functools
import math

import jax
import jax.numpy as jnp
from jax import lax
from jax.experimental import pallas as pl
from jax.experimental.pallas import tpu as pltpu
from jax.sharding import PartitionSpec as P

F32 = jnp.float32
BF16 = jnp.bfloat16
NT = (((1,), (1,)), ((), ()))
TN = (((0,), (0,)), ((), ()))


def mm(a, b, dims=(((1,), (0,)), ((), ()))):
    return lax.dot_general(a, b, dims, preferred_element_type=F32)


def one_hot(cond):
    return jnp.where(cond, 1.0, 0.0).astype(BF16)


def local_kernel(
    rim_ref, w1_ref, w2_ref, cot_ref, out_ref, vf, lhs, s_ref, slope_ref, cols, lower,
    *, cin, hx, hy, hz, g_lane, scale_first, scale_second,
):
    nx, ny = hx + 2, hy + 2
    row = ny * hz
    c1 = w1_ref.shape[0]
    win = 16 * cin
    pairs = nx * ny // 2
    lanes = 2 * hz

    vf[...] = rim_ref[...].astype(F32)
    ri = lax.broadcasted_iota(jnp.int32, (2 * lanes, 4 * lanes), 0)
    ci = lax.broadcasted_iota(jnp.int32, (2 * lanes, 4 * lanes), 1)
    sel = one_hot(
        ((ri // lanes) == ((ci % lanes) // hz))
        & ((ri % lanes) == 2 * (ci % hz) + ci // lanes - 1)
    )
    for p in range(pairs):
        for half in range(2):
            cell = 2 * p + half
            cx, cy = cell // ny, cell % ny
            for dx in range(4):
                lhs[
                    p * win + dx * 4 * cin : p * win + (dx + 1) * 4 * cin,
                    half * lanes : (half + 1) * lanes,
                ] = vf[2 * cx + dx, 2 * cin * cy : 2 * cin * cy + 4 * cin, :].astype(BF16)
    picked = mm(lhs[...], sel).astype(BF16)
    for p in range(pairs):
        for o in range(4):
            s_ref[o * win : (o + 1) * win, p * lanes : (p + 1) * lanes] = picked[
                p * win : (p + 1) * win, o * lanes : (o + 1) * lanes
            ]

    wide = w1_ref.shape[1]
    fi = lax.broadcasted_iota(jnp.int32, (4 * win, wide), 0)
    ni = lax.broadcasted_iota(jnp.int32, (4 * win, wide), 1)
    k = ni // cin
    base = (k % 3) * win + (k // 9) * 4 * cin + ((k // 3) % 3) * cin + ni % cin
    diff = fi - base
    folds = [
        one_hot(diff == fz * win + fx * 4 * cin + fy * cin)
        for fx in range(2)
        for fy in range(2)
        for fz in range(2)
    ]
    w1 = w1_ref[...]
    toeplitz = jnp.concatenate([mm(w1, f, NT).astype(BF16) for f in folds], axis=0)

    ix, iy = lax.axis_index("sx"), lax.axis_index("sy")
    last_x, last_y = lax.axis_size("sx") - 1, lax.axis_size("sy") - 1
    lane = lax.broadcasted_iota(jnp.int32, (1, row), 1)
    low_y = jnp.where(iy == 0, hz, 0)
    high_y = jnp.where(iy == last_y, row - hz, row)
    mask_y = jnp.where((lane >= low_y) & (lane < high_y), 1.0, 0.0).astype(F32)
    not_first = jnp.where(lane % hz == 0, 0.0, 1.0).astype(F32)
    not_last = jnp.where(lane % hz == hz - 1, 0.0, 1.0).astype(F32)

    own = hy * hz
    for cx in range(nx):
        here = slice(cx * row, (cx + 1) * row)
        pre = mm(toeplitz, s_ref[:, here])
        t = jnp.exp(-jnp.abs(pre))
        r = 1.0 / (1.0 + t)
        soft = jnp.maximum(pre, 0.0) + jnp.log(1.0 + t)
        sig = jnp.where(pre >= 0, r, t * r)
        hidden = (0.3 * pre + 0.7 * soft).astype(BF16).astype(F32)
        mask = mask_y
        if cx == 0:
            mask = mask * jnp.where(ix == 0, 0.0, 1.0)
        if cx == nx - 1:
            mask = mask * jnp.where(ix == last_x, 0.0, 1.0)
        slope_ref[:, here] = (0.3 + 0.7 * sig) * (mask * 0.125)
        total = hidden[0:c1]
        for s in range(1, 8):
            total = total + hidden[s * c1 : (s + 1) * c1]
        pooled = total * (mask * 0.125)
        three = jnp.concatenate(
            [
                pltpu.roll(pooled, 1, 1) * not_first,
                pooled,
                pltpu.roll(pooled, row - 1, 1) * not_last,
            ],
            axis=0,
        )
        odd = pltpu.roll(three, row - hz, 1).astype(BF16)
        even = three.astype(BF16)
        for a in range(3):
            x = cx - a
            if 0 <= x < hx:
                for b in range(3):
                    at = 3 * c1 * (3 * a + b)
                    piece = odd[:, 0:own] if b == 1 else even[:, b * hz : b * hz + own]
                    cols[at : at + 3 * c1, x * own : (x + 1) * own] = piece

    w2 = w2_ref[...]
    pre2 = mm(w2, cols[...])
    t = jnp.exp(-jnp.abs(pre2))
    r = 1.0 / (1.0 + t)
    slope2 = 0.3 + 0.7 * jnp.where(pre2 >= 0, r, t * r)
    back = (cot_ref[...].astype(F32) * slope2).astype(BF16)
    spread = mm(w2, back, TN)
    second = mm(back, cols[...], NT) * scale_second
    out_ref[...] = jnp.zeros(out_ref.shape, out_ref.dtype)
    out_ref[:, 0 : second.shape[1]] = second.astype(out_ref.dtype)

    for cx in range(nx):
        here = slice(cx * row, (cx + 1) * row)
        blocks = []
        for b in range(3):
            acc = None
            for a in range(3):
                x = cx - a
                if 0 <= x < hx:
                    at = 3 * c1 * (3 * a + b)
                    piece = spread[at : at + 3 * c1, x * own : (x + 1) * own]
                    acc = piece if acc is None else acc + piece
            blocks.append(acc)
        gap = jnp.zeros((3 * c1, 2 * hz), F32)
        grown = (
            jnp.concatenate([blocks[0], gap], axis=1)
            + jnp.concatenate([gap, blocks[2]], axis=1)
            + pltpu.roll(jnp.concatenate([blocks[1], gap], axis=1), hz, 1)
        )
        up = (
            pltpu.roll(grown[0:c1], row - 1, 1) * not_last
            + grown[c1 : 2 * c1]
            + pltpu.roll(grown[2 * c1 : 3 * c1], 1, 1) * not_first
        )
        for s in range(8):
            lower[s * c1 : (s + 1) * c1, here] = (
                up * slope_ref[s * c1 : (s + 1) * c1, here]
            ).astype(BF16)

    products = mm(lower[...], s_ref[...], NT)
    high = products.astype(BF16)
    low = (products - high.astype(F32)).astype(BF16)
    first = jnp.zeros((c1, wide), F32)
    for s in range(8):
        part = slice(s * c1, (s + 1) * c1)
        first = first + mm(high[part], folds[s]) + mm(low[part], folds[s])
    out_ref[0:c1, g_lane : g_lane + wide] = (first * scale_first).astype(out_ref.dtype)


def exchange(block, axis, dim, width):
    count = lax.axis_size(axis)
    size = block.shape[dim]
    top = lax.slice_in_dim(block, size - width, size, axis=dim)
    bottom = lax.slice_in_dim(block, 0, width, axis=dim)
    if count == 2:
        first = lax.axis_index(axis) == 0
        got = lax.ppermute(jnp.where(first, top, bottom), axis, [(0, 1), (1, 0)])
        none = jnp.zeros_like(got)
        low, high = jnp.where(first, none, got), jnp.where(first, got, none)
    else:
        ahead = [(i, i + 1) for i in range(count - 1)]
        low = lax.ppermute(top, axis, ahead)
        high = lax.ppermute(bottom, axis, [(j, i) for i, j in ahead])
    return jnp.concatenate([low, block, high], axis=dim)


def total_over(value, axes):
    for axis in axes:
        count = lax.axis_size(axis)
        if count & (count - 1):
            value = lax.psum(value.astype(F32), axis).astype(value.dtype)
            continue
        step = 1
        while step < count:
            other = lax.ppermute(value, axis, [(i, i ^ step) for i in range(count)])
            value = (value.astype(F32) + other.astype(F32)).astype(value.dtype)
            step *= 2
    return value


def shards(volume, first_weight, second_weight, cotangent):
    samples, cin, wx, wy, wz = volume.shape
    hx, hy, hz = wx // 2, wy // 2, wz // 2
    c1, wide = first_weight.shape
    c2, tall = second_weight.shape
    devices = lax.axis_size("dp") * lax.axis_size("sx") * lax.axis_size("sy")
    coarse = samples * hx * hy * hz * devices
    g_lane = -(-tall // 128) * 128
    width = g_lane + -(-wide // 128) * 128
    nx, ny = hx + 2, hy + 2
    lane = nx * ny * hz
    win = 16 * cin

    block = volume[0].transpose(1, 2, 0, 3)
    rim = exchange(exchange(block, "sy", 1, 3), "sx", 0, 3)
    rim = rim.reshape(wx + 6, (wy + 6) * cin, wz)
    cot = cotangent[0].reshape(c2, hx * hy * hz)

    body = functools.partial(
        local_kernel, cin=cin, hx=hx, hy=hy, hz=hz, g_lane=g_lane,
        scale_first=1.0 / math.sqrt(coarse * 8), scale_second=1.0 / math.sqrt(coarse),
    )
    part = pl.pallas_call(
        body,
        out_shape=jax.ShapeDtypeStruct((c2, width), BF16),
        scratch_shapes=[
            pltpu.VMEM(rim.shape, F32),
            pltpu.VMEM((nx * ny // 2 * win, 2 * wz), BF16),
            pltpu.VMEM((4 * win, lane), BF16),
            pltpu.VMEM((8 * c1, lane), F32),
            pltpu.VMEM((tall, hx * hy * hz), BF16),
            pltpu.VMEM((8 * c1, lane), BF16),
        ],
        name="local_step",
    )(rim, first_weight, second_weight, cot)
    total = total_over(part, ("sx", "sy", "dp")).astype(F32)
    return total[:c1, g_lane : g_lane + wide], total[:, :tall]


def solution(mesh):
    return jax.shard_map(
        shards,
        mesh=mesh,
        in_specs=(P("dp", None, "sx", "sy", None), P(), P(), P("dp", None, "sx", "sy", None)),
        out_specs=(P(), P()),
        check_vma=False,
    )
```

```python
import functools
import math

import jax
import jax.numpy as jnp
from jax import lax
from jax.experimental import pallas as pl
from jax.experimental.pallas import tpu as pltpu
from jax.sharding import PartitionSpec as P

F32 = jnp.float32
BF16 = jnp.bfloat16
NT = (((1,), (1,)), ((), ()))
RIM = 3
TN = (((0,), (0,)), ((), ()))


def mm(a, b, dims=(((1,), (0,)), ((), ()))):
    return lax.dot_general(a, b, dims, preferred_element_type=F32)


def one_hot(cond):
    return jnp.where(cond, 1.0, 0.0).astype(BF16)


def local_kernel(
    block_ref, near_ref, far_ref, side_ref, diag_ref, w1_ref, w2_ref, cot_ref, keep_ref, send_ref,
    vf, lhs, s_ref, slope_ref, cols, lower,
    *, cin, hx, hy, hz, g_lane, scale_first, scale_second,
):
    nx, ny = hx + 2, hy + 2
    row = ny * hz
    c1 = w1_ref.shape[0]
    win = 16 * cin
    pairs = nx * ny // 2
    lanes = 2 * hz

    ix, iy = lax.axis_index("sx"), lax.axis_index("sy")
    last_x, last_y = lax.axis_size("sx") - 1, lax.axis_size("sy") - 1
    odd_x = ix % 2
    wx, rows = 2 * hx, 2 * hy * cin
    lip = RIM * cin
    near_at = jnp.where(odd_x == 1, 0, RIM + wx)
    far_at = RIM + wx - near_at
    vf[RIM : RIM + wx, lip : lip + rows, :] = block_ref[...].astype(F32)
    vf[pl.ds(near_at, RIM), lip : lip + rows, :] = near_ref[...].astype(F32)
    vf[pl.ds(far_at, RIM), lip : lip + rows, :] = far_ref[...].astype(F32)
    for at, count, piece in (
        (RIM, wx, side_ref[0:wx]),
        (near_at, RIM, side_ref[wx : wx + RIM]),
        (far_at, RIM, diag_ref[...]),
    ):
        piece = piece.astype(F32)
        vf[pl.ds(at, count), 0:lip, :] = jnp.where(iy == 0, 0.0, piece)
        vf[pl.ds(at, count), lip + rows : 2 * lip + rows, :] = jnp.where(iy == 0, piece, 0.0)
    ri = lax.broadcasted_iota(jnp.int32, (2 * lanes, 4 * lanes), 0)
    ci = lax.broadcasted_iota(jnp.int32, (2 * lanes, 4 * lanes), 1)
    sel = one_hot(
        ((ri // lanes) == ((ci % lanes) // hz))
        & ((ri % lanes) == 2 * (ci % hz) + ci // lanes - 1)
    )
    for p in range(pairs):
        for half in range(2):
            cell = 2 * p + half
            cx, cy = cell // ny, cell % ny
            for dx in range(4):
                lhs[
                    p * win + dx * 4 * cin : p * win + (dx + 1) * 4 * cin,
                    half * lanes : (half + 1) * lanes,
                ] = vf[2 * cx + dx, 2 * cin * cy : 2 * cin * cy + 4 * cin, :].astype(BF16)
    picked = mm(lhs[...], sel).astype(BF16)
    for p in range(pairs):
        for o in range(4):
            s_ref[o * win : (o + 1) * win, p * lanes : (p + 1) * lanes] = picked[
                p * win : (p + 1) * win, o * lanes : (o + 1) * lanes
            ]

    wide = w1_ref.shape[1]
    fi = lax.broadcasted_iota(jnp.int32, (4 * win, wide), 0)
    ni = lax.broadcasted_iota(jnp.int32, (4 * win, wide), 1)
    k = ni // cin
    base = (k % 3) * win + (k // 9) * 4 * cin + ((k // 3) % 3) * cin + ni % cin
    diff = fi - base
    folds = [
        one_hot(diff == fz * win + fx * 4 * cin + fy * cin)
        for fx in range(2)
        for fy in range(2)
        for fz in range(2)
    ]
    w1 = w1_ref[...]
    toeplitz = jnp.concatenate([mm(w1, f, NT).astype(BF16) for f in folds], axis=0)

    lane = lax.broadcasted_iota(jnp.int32, (1, row), 1)
    low_y = jnp.where(iy == 0, hz, 0)
    high_y = jnp.where(iy == last_y, row - hz, row)
    mask_y = jnp.where((lane >= low_y) & (lane < high_y), 1.0, 0.0).astype(F32)
    not_first = jnp.where(lane % hz == 0, 0.0, 1.0).astype(F32)
    not_last = jnp.where(lane % hz == hz - 1, 0.0, 1.0).astype(F32)

    own = hy * hz
    for cx in range(nx):
        here = slice(cx * row, (cx + 1) * row)
        pre = mm(toeplitz, s_ref[:, here])
        t = jnp.exp(-jnp.abs(pre))
        r = 1.0 / (1.0 + t)
        soft = jnp.maximum(pre, 0.0) + jnp.log(1.0 + t)
        sig = jnp.where(pre >= 0, r, t * r)
        hidden = (0.3 * pre + 0.7 * soft).astype(BF16).astype(F32)
        mask = mask_y
        if cx == 0:
            mask = mask * jnp.where(ix == 0, 0.0, 1.0)
        if cx == nx - 1:
            mask = mask * jnp.where(ix == last_x, 0.0, 1.0)
        slope_ref[:, here] = (0.3 + 0.7 * sig) * (mask * 0.125)
        total = hidden[0:c1]
        for s in range(1, 8):
            total = total + hidden[s * c1 : (s + 1) * c1]
        pooled = total * (mask * 0.125)
        three = jnp.concatenate(
            [
                pltpu.roll(pooled, 1, 1) * not_first,
                pooled,
                pltpu.roll(pooled, row - 1, 1) * not_last,
            ],
            axis=0,
        )
        odd = pltpu.roll(three, row - hz, 1).astype(BF16)
        even = three.astype(BF16)
        for a in range(3):
            x = cx - a
            if 0 <= x < hx:
                for b in range(3):
                    at = 3 * c1 * (3 * a + b)
                    piece = odd[:, 0:own] if b == 1 else even[:, b * hz : b * hz + own]
                    cols[at : at + 3 * c1, x * own : (x + 1) * own] = piece

    w2 = w2_ref[...]
    pre2 = mm(w2, cols[...])
    t = jnp.exp(-jnp.abs(pre2))
    r = 1.0 / (1.0 + t)
    slope2 = 0.3 + 0.7 * jnp.where(pre2 >= 0, r, t * r)
    back = (cot_ref[...].astype(F32) * slope2).astype(BF16)
    spread = mm(w2, back, TN)
    second = mm(back, cols[...], NT) * scale_second
    tall = second.shape[1]
    half = second.shape[0] // 2
    is_odd = odd_x == 1
    keep_ref[...] = jnp.zeros(keep_ref.shape, keep_ref.dtype)
    send_ref[...] = jnp.zeros(send_ref.shape, send_ref.dtype)
    keep_ref[:, 0:tall] = jnp.where(is_odd, second[half:], second[:half])
    send_ref[:, 0:tall] = jnp.where(is_odd, second[:half], second[half:]).astype(BF16)

    for cx in range(nx):
        here = slice(cx * row, (cx + 1) * row)
        blocks = []
        for b in range(3):
            acc = None
            for a in range(3):
                x = cx - a
                if 0 <= x < hx:
                    at = 3 * c1 * (3 * a + b)
                    piece = spread[at : at + 3 * c1, x * own : (x + 1) * own]
                    acc = piece if acc is None else acc + piece
            blocks.append(acc)
        gap = jnp.zeros((3 * c1, 2 * hz), F32)
        grown = (
            jnp.concatenate([blocks[0], gap], axis=1)
            + jnp.concatenate([gap, blocks[2]], axis=1)
            + pltpu.roll(jnp.concatenate([blocks[1], gap], axis=1), hz, 1)
        )
        up = (
            pltpu.roll(grown[0:c1], row - 1, 1) * not_last
            + grown[c1 : 2 * c1]
            + pltpu.roll(grown[2 * c1 : 3 * c1], 1, 1) * not_first
        )
        for s in range(8):
            lower[s * c1 : (s + 1) * c1, here] = (
                up * slope_ref[s * c1 : (s + 1) * c1, here]
            ).astype(BF16)

    products = mm(lower[...], s_ref[...], NT)
    high = products.astype(BF16)
    low = (products - high.astype(F32)).astype(BF16)
    first = jnp.zeros((c1, wide), F32)
    for s in range(8):
        part = slice(s * c1, (s + 1) * c1)
        first = first + mm(high[part], folds[s]) + mm(low[part], folds[s])
    first = first * scale_first
    keep_ref[0:c1, g_lane : g_lane + wide] = jnp.where(is_odd, 0.0, first)
    send_ref[0:c1, g_lane : g_lane + wide] = jnp.where(is_odd, first, 0.0).astype(BF16)


def join_kernel(mine_ref, other_ref, first_ref, second_ref, *, g_lane):
    is_odd = lax.axis_index("sx") % 2 == 1
    mine, other = mine_ref[...].astype(F32), other_ref[...].astype(F32)
    upper = jnp.where(is_odd, other, mine)
    half = mine.shape[0]
    tall = second_ref.shape[1]
    c1, wide = first_ref.shape
    second_ref[0:half, :] = upper[:, 0:tall]
    second_ref[half:, :] = jnp.where(is_odd, mine, other)[:, 0:tall]
    first_ref[...] = upper[0:c1, g_lane : g_lane + wide]


def swap(value, axes, mask):
    count = lax.axis_size(axes)
    return lax.ppermute(value, axes, [(i, i ^ mask) for i in range(count)])


def total_over(value, axes, masks):
    for at in range(0, len(masks), 2):
        pair = masks[at : at + 2]
        if len(pair) == 1:
            value = (value.astype(F32) + swap(value, axes, pair[0]).astype(F32)).astype(BF16)
            continue
        m, n = pair
        one, two, three = (swap(value, axes, x).astype(F32) for x in (m, n, m ^ n))
        value = ((value.astype(F32) + one) + (two + three)).astype(BF16)
    return value


def bits(count):
    return [1 << i for i in range(count.bit_length() - 1)]


def shards(volume, first_weight, second_weight, cotangent):
    samples, cin, wx, wy, wz = volume.shape
    hx, hy, hz = wx // 2, wy // 2, wz // 2
    c1, wide = first_weight.shape
    c2, tall = second_weight.shape
    devices = lax.axis_size("dp") * lax.axis_size("sx") * lax.axis_size("sy")
    coarse = samples * hx * hy * hz * devices
    g_lane = -(-tall // 128) * 128
    width = g_lane + -(-wide // 128) * 128
    nx, ny = hx + 2, hy + 2
    lane = nx * ny * hz
    win = 16 * cin

    count_x, count_y = lax.axis_size("sx"), lax.axis_size("sy")
    assert count_y == 2 and count_x & (count_x - 1) == 0 and 2 * c1 == c2
    odd_x = lax.axis_index("sx") % 2 == 1
    low_y = lax.axis_index("sy") == 0
    lip = RIM * cin
    block = volume[0].transpose(1, 2, 0, 3).reshape(wx, wy * cin, wz)

    def rim_y(piece):
        return jnp.where(low_y, piece[:, -lip:], piece[:, :lip])

    inner = jnp.where(odd_x, block[:RIM], block[-RIM:])
    outer = jnp.where(odd_x, block[-RIM:], block[:RIM])
    near = swap(inner, "sx", 1)
    pairs = [(i, i + 1) for i in range(1, count_x - 1, 2)]
    pairs = pairs + [(j, i) for i, j in pairs]
    far = lax.ppermute(outer, "sx", pairs)
    crossed = [(2 * i + t, 2 * j + 1 - t) for i, j in pairs for t in range(2)]
    diag = lax.ppermute(rim_y(outer), ("sx", "sy"), crossed)
    side = swap(jnp.concatenate([rim_y(block), rim_y(near)], axis=0), "sy", 1)
    cot = cotangent[0].reshape(c2, hx * hy * hz)

    body = functools.partial(
        local_kernel, cin=cin, hx=hx, hy=hy, hz=hz, g_lane=g_lane,
        scale_first=1.0 / math.sqrt(coarse * 8), scale_second=1.0 / math.sqrt(coarse),
    )
    keep, send = pl.pallas_call(
        body,
        out_shape=(
            jax.ShapeDtypeStruct((c2 // 2, width), F32),
            jax.ShapeDtypeStruct((c2 // 2, width), BF16),
        ),
        scratch_shapes=[
            pltpu.VMEM((wx + 2 * RIM, (wy + 2 * RIM) * cin, wz), F32),
            pltpu.VMEM((nx * ny // 2 * win, 2 * wz), BF16),
            pltpu.VMEM((4 * win, lane), BF16),
            pltpu.VMEM((8 * c1, lane), F32),
            pltpu.VMEM((tall, hx * hy * hz), BF16),
            pltpu.VMEM((8 * c1, lane), BF16),
        ],
        name="local_step",
    )(block, near, far, side, diag, first_weight, second_weight, cot)
    mine = (keep + swap(send, "sx", 1).astype(F32)).astype(BF16)
    mine = total_over(mine, ("sx", "sy"), [1] + [2 * m for m in bits(count_x)[1:]])
    mine = total_over(mine, ("dp",), bits(lax.axis_size("dp")))
    return pl.pallas_call(
        functools.partial(join_kernel, g_lane=g_lane),
        out_shape=(
            jax.ShapeDtypeStruct((c1, wide), F32),
            jax.ShapeDtypeStruct((c2, tall), F32),
        ),
        name="join",
    )(mine, swap(mine, "sx", 1))


def solution(mesh):
    return jax.shard_map(
        shards,
        mesh=mesh,
        in_specs=(P("dp", None, "sx", "sy", None), P(), P(), P("dp", None, "sx", "sy", None)),
        out_specs=(P(), P()),
        check_vma=False,
    )
```

```python
import functools
import math

import jax
import jax.numpy as jnp
from jax import lax
from jax.experimental import pallas as pl
from jax.experimental.pallas import tpu as pltpu
from jax.sharding import PartitionSpec as P

F32 = jnp.float32
BF16 = jnp.bfloat16
NT = (((1,), (1,)), ((), ()))
RIM = 3
TN = (((0,), (0,)), ((), ()))


def mm(a, b, dims=(((1,), (0,)), ((), ()))):
    return lax.dot_general(a, b, dims, preferred_element_type=F32)


def one_hot(cond):
    return jnp.where(cond, 1.0, 0.0).astype(BF16)


def local_kernel(
    block_ref, near_ref, far_ref, side_ref, diag_ref, w1_ref, w2_ref, cot_ref, keep_ref, send_ref,
    vf, lhs, s_ref, slope_ref, cols, lower,
    *, cin, hx, hy, hz, g_lane, scale_first, scale_second,
):
    nx, ny = hx + 2, hy + 2
    row = ny * hz
    c1 = w1_ref.shape[0]
    win = 16 * cin
    pairs = nx * ny // 2
    lanes = 2 * hz

    ix, iy = lax.axis_index("sx"), lax.axis_index("sy")
    last_x, last_y = lax.axis_size("sx") - 1, lax.axis_size("sy") - 1
    odd_x = ix % 2
    wx, rows = 2 * hx, 2 * hy * cin
    lip = RIM * cin
    near_at = jnp.where(odd_x == 1, 0, RIM + wx)
    far_at = RIM + wx - near_at
    vf[RIM : RIM + wx, lip : lip + rows, :] = block_ref[...].astype(F32)
    vf[pl.ds(near_at, RIM), lip : lip + rows, :] = near_ref[...].astype(F32)
    vf[pl.ds(far_at, RIM), lip : lip + rows, :] = far_ref[...].astype(F32)
    for at, count, piece in (
        (RIM, wx, side_ref[0:wx]),
        (near_at, RIM, side_ref[wx : wx + RIM]),
        (far_at, RIM, diag_ref[...]),
    ):
        piece = piece.astype(F32)
        vf[pl.ds(at, count), 0:lip, :] = jnp.where(iy == 0, 0.0, piece)
        vf[pl.ds(at, count), lip + rows : 2 * lip + rows, :] = jnp.where(iy == 0, piece, 0.0)
    ri = lax.broadcasted_iota(jnp.int32, (2 * lanes, 4 * lanes), 0)
    ci = lax.broadcasted_iota(jnp.int32, (2 * lanes, 4 * lanes), 1)
    sel = one_hot(
        ((ri // lanes) == ((ci % lanes) // hz))
        & ((ri % lanes) == 2 * (ci % hz) + ci // lanes - 1)
    )
    for p in range(pairs):
        for half in range(2):
            cell = 2 * p + half
            cx, cy = cell // ny, cell % ny
            for dx in range(4):
                lhs[
                    p * win + dx * 4 * cin : p * win + (dx + 1) * 4 * cin,
                    half * lanes : (half + 1) * lanes,
                ] = vf[2 * cx + dx, 2 * cin * cy : 2 * cin * cy + 4 * cin, :].astype(BF16)
    picked = mm(lhs[...], sel).astype(BF16)
    for p in range(pairs):
        for o in range(4):
            s_ref[o * win : (o + 1) * win, p * lanes : (p + 1) * lanes] = picked[
                p * win : (p + 1) * win, o * lanes : (o + 1) * lanes
            ]

    wide = w1_ref.shape[1]
    fi = lax.broadcasted_iota(jnp.int32, (4 * win, wide), 0)
    ni = lax.broadcasted_iota(jnp.int32, (4 * win, wide), 1)
    k = ni // cin
    base = (k % 3) * win + (k // 9) * 4 * cin + ((k // 3) % 3) * cin + ni % cin
    diff = fi - base
    folds = [
        one_hot(diff == fz * win + fx * 4 * cin + fy * cin)
        for fx in range(2)
        for fy in range(2)
        for fz in range(2)
    ]
    w1 = w1_ref[...]
    toeplitz = jnp.concatenate([mm(w1, f, NT).astype(BF16) for f in folds], axis=0)

    lane = lax.broadcasted_iota(jnp.int32, (1, row), 1)
    low_y = jnp.where(iy == 0, hz, 0)
    high_y = jnp.where(iy == last_y, row - hz, row)
    mask_y = jnp.where((lane >= low_y) & (lane < high_y), 1.0, 0.0).astype(F32)
    not_first = jnp.where(lane % hz == 0, 0.0, 1.0).astype(F32)
    not_last = jnp.where(lane % hz == hz - 1, 0.0, 1.0).astype(F32)

    own = hy * hz
    for cx in range(nx):
        here = slice(cx * row, (cx + 1) * row)
        pre = mm(toeplitz, s_ref[:, here])
        t = jnp.exp(-jnp.abs(pre))
        r = 1.0 / (1.0 + t)
        soft = jnp.maximum(pre, 0.0) + jnp.log(1.0 + t)
        sig = jnp.where(pre >= 0, r, t * r)
        hidden = (0.3 * pre + 0.7 * soft).astype(BF16).astype(F32)
        mask = mask_y
        if cx == 0:
            mask = mask * jnp.where(ix == 0, 0.0, 1.0)
        if cx == nx - 1:
            mask = mask * jnp.where(ix == last_x, 0.0, 1.0)
        slope_ref[:, here] = (0.3 + 0.7 * sig) * (mask * 0.125)
        total = hidden[0:c1]
        for s in range(1, 8):
            total = total + hidden[s * c1 : (s + 1) * c1]
        pooled = total * (mask * 0.125)
        three = jnp.concatenate(
            [
                pltpu.roll(pooled, 1, 1) * not_first,
                pooled,
                pltpu.roll(pooled, row - 1, 1) * not_last,
            ],
            axis=0,
        )
        odd = pltpu.roll(three, row - hz, 1).astype(BF16)
        even = three.astype(BF16)
        for a in range(3):
            x = cx - a
            if 0 <= x < hx:
                for b in range(3):
                    at = 3 * c1 * (3 * a + b)
                    piece = odd[:, 0:own] if b == 1 else even[:, b * hz : b * hz + own]
                    cols[at : at + 3 * c1, x * own : (x + 1) * own] = piece

    w2 = w2_ref[...]
    pre2 = mm(w2, cols[...])
    t = jnp.exp(-jnp.abs(pre2))
    r = 1.0 / (1.0 + t)
    slope2 = 0.3 + 0.7 * jnp.where(pre2 >= 0, r, t * r)
    back = (cot_ref[...].astype(F32) * slope2).astype(BF16)
    spread = mm(w2, back, TN)
    second = mm(back, cols[...], NT) * scale_second
    tall = second.shape[1]
    half = second.shape[0] // 2
    is_odd = odd_x == 1
    keep_ref[...] = jnp.zeros(keep_ref.shape, keep_ref.dtype)
    send_ref[...] = jnp.zeros(send_ref.shape, send_ref.dtype)
    keep_ref[:, 0:tall] = jnp.where(is_odd, second[half:], second[:half])
    send_ref[:, 0:tall] = jnp.where(is_odd, second[:half], second[half:]).astype(BF16)

    for cx in range(nx):
        here = slice(cx * row, (cx + 1) * row)
        blocks = []
        for b in range(3):
            acc = None
            for a in range(3):
                x = cx - a
                if 0 <= x < hx:
                    at = 3 * c1 * (3 * a + b)
                    piece = spread[at : at + 3 * c1, x * own : (x + 1) * own]
                    acc = piece if acc is None else acc + piece
            blocks.append(acc)
        gap = jnp.zeros((3 * c1, 2 * hz), F32)
        grown = (
            jnp.concatenate([blocks[0], gap], axis=1)
            + jnp.concatenate([gap, blocks[2]], axis=1)
            + pltpu.roll(jnp.concatenate([blocks[1], gap], axis=1), hz, 1)
        )
        up = (
            pltpu.roll(grown[0:c1], row - 1, 1) * not_last
            + grown[c1 : 2 * c1]
            + pltpu.roll(grown[2 * c1 : 3 * c1], 1, 1) * not_first
        )
        for s in range(8):
            lower[s * c1 : (s + 1) * c1, here] = (
                up * slope_ref[s * c1 : (s + 1) * c1, here]
            ).astype(BF16)

    products = mm(lower[...], s_ref[...], NT)
    high = products.astype(BF16)
    low = (products - high.astype(F32)).astype(BF16)
    first = jnp.zeros((c1, wide), F32)
    for s in range(8):
        part = slice(s * c1, (s + 1) * c1)
        first = first + mm(high[part], folds[s]) + mm(low[part], folds[s])
    first = first * scale_first
    keep_ref[0:c1, g_lane : g_lane + wide] = jnp.where(is_odd, 0.0, first)
    send_ref[0:c1, g_lane : g_lane + wide] = jnp.where(is_odd, first, 0.0).astype(BF16)


def join_kernel(mine_ref, other_ref, first_ref, second_ref, *, g_lane):
    is_odd = lax.axis_index("sx") % 2 == 1
    mine, other = mine_ref[...].astype(F32), other_ref[...].astype(F32)
    upper = jnp.where(is_odd, other, mine)
    half = mine.shape[0]
    tall = second_ref.shape[1]
    c1, wide = first_ref.shape
    second_ref[0:half, :] = upper[:, 0:tall]
    second_ref[half:, :] = jnp.where(is_odd, mine, other)[:, 0:tall]
    first_ref[...] = upper[0:c1, g_lane : g_lane + wide]


def swap(value, axes, mask):
    count = lax.axis_size(axes)
    return lax.ppermute(value, axes, [(i, i ^ mask) for i in range(count)])


def total_over(value, axes, masks):
    for at in range(0, len(masks), 2):
        pair = masks[at : at + 2]
        if len(pair) == 1:
            value = (value.astype(F32) + swap(value, axes, pair[0]).astype(F32)).astype(BF16)
            continue
        m, n = pair
        one, two, three = (swap(value, axes, x).astype(F32) for x in (m, n, m ^ n))
        value = ((value.astype(F32) + one) + (two + three)).astype(BF16)
    return value


def near_core(value):
    return pltpu.with_memory_space_constraint(value, pltpu.VMEM)


def bits(count):
    return [1 << i for i in range(count.bit_length() - 1)]


def shards(volume, first_weight, second_weight, cotangent):
    samples, cin, wx, wy, wz = volume.shape
    hx, hy, hz = wx // 2, wy // 2, wz // 2
    c1, wide = first_weight.shape
    c2, tall = second_weight.shape
    devices = lax.axis_size("dp") * lax.axis_size("sx") * lax.axis_size("sy")
    coarse = samples * hx * hy * hz * devices
    g_lane = -(-tall // 128) * 128
    width = g_lane + -(-wide // 128) * 128
    nx, ny = hx + 2, hy + 2
    lane = nx * ny * hz
    win = 16 * cin

    count_x, count_y = lax.axis_size("sx"), lax.axis_size("sy")
    assert count_y == 2 and count_x & (count_x - 1) == 0 and 2 * c1 == c2
    odd_x = lax.axis_index("sx") % 2 == 1
    low_y = lax.axis_index("sy") == 0
    lip = RIM * cin
    block = volume[0].transpose(1, 2, 0, 3).reshape(wx, wy * cin, wz)

    def rim_y(piece):
        return jnp.where(low_y, piece[:, -lip:], piece[:, :lip])

    inner = jnp.where(odd_x, block[:RIM], block[-RIM:])
    outer = jnp.where(odd_x, block[-RIM:], block[:RIM])
    near = swap(inner, "sx", 1)
    pairs = [(i, i + 1) for i in range(1, count_x - 1, 2)]
    pairs = pairs + [(j, i) for i, j in pairs]
    far = lax.ppermute(outer, "sx", pairs)
    crossed = [(2 * i + t, 2 * j + 1 - t) for i, j in pairs for t in range(2)]
    diag = lax.ppermute(rim_y(outer), ("sx", "sy"), crossed)
    side = swap(jnp.concatenate([rim_y(block), rim_y(near)], axis=0), "sy", 1)
    cot = cotangent[0].reshape(c2, hx * hy * hz)

    body = functools.partial(
        local_kernel, cin=cin, hx=hx, hy=hy, hz=hz, g_lane=g_lane,
        scale_first=1.0 / math.sqrt(coarse * 8), scale_second=1.0 / math.sqrt(coarse),
    )
    keep, send = pl.pallas_call(
        body,
        out_shape=(
            pltpu.VMEM((c2 // 2, width), F32),
            pltpu.VMEM((c2 // 2, width), BF16),
        ),
        scratch_shapes=[
            pltpu.VMEM((wx + 2 * RIM, (wy + 2 * RIM) * cin, wz), F32),
            pltpu.VMEM((nx * ny // 2 * win, 2 * wz), BF16),
            pltpu.VMEM((4 * win, lane), BF16),
            pltpu.VMEM((8 * c1, lane), F32),
            pltpu.VMEM((tall, hx * hy * hz), BF16),
            pltpu.VMEM((8 * c1, lane), BF16),
        ],
        name="local_step",
    )(*map(near_core, (block, near, far, side, diag)), first_weight, second_weight, near_core(cot))
    mine = (keep + swap(send, "sx", 1).astype(F32)).astype(BF16)
    mine = total_over(mine, ("sx", "sy"), [1] + [2 * m for m in bits(count_x)[1:]])
    mine = total_over(mine, ("dp",), bits(lax.axis_size("dp")))
    return pl.pallas_call(
        functools.partial(join_kernel, g_lane=g_lane),
        out_shape=(
            jax.ShapeDtypeStruct((c1, wide), F32),
            jax.ShapeDtypeStruct((c2, tall), F32),
        ),
        name="join",
    )(near_core(mine), near_core(swap(mine, "sx", 1)))


def solution(mesh):
    return jax.shard_map(
        shards,
        mesh=mesh,
        in_specs=(P("dp", None, "sx", "sy", None), P(), P(), P("dp", None, "sx", "sy", None)),
        out_specs=(P(), P()),
        check_vma=False,
    )
```

```python
import functools
import math

import jax
import jax.numpy as jnp
from jax import lax
from jax.experimental import pallas as pl
from jax.experimental.pallas import tpu as pltpu
from jax.sharding import PartitionSpec as P

F32 = jnp.float32
BF16 = jnp.bfloat16
NT = (((1,), (1,)), ((), ()))
RIM = 3
TN = (((0,), (0,)), ((), ()))


def mm(a, b, dims=(((1,), (0,)), ((), ()))):
    return lax.dot_general(a, b, dims, preferred_element_type=F32)


def one_hot(cond):
    return jnp.where(cond, 1.0, 0.0).astype(BF16)


def local_kernel(
    block_ref, near_ref, far_ref, side_ref, w1_ref, w2_ref, cot_ref, keep_ref, send_ref,
    vf, lhs, s_ref, slope_ref, cols, lower,
    *, cin, hx, hy, hz, g_lane, scale_first, scale_second,
):
    nx, ny = hx + 2, hy + 2
    row = ny * hz
    c1 = w1_ref.shape[0]
    win = 16 * cin
    pairs = nx * ny // 2
    lanes = 2 * hz

    ix, iy = lax.axis_index("sx"), lax.axis_index("sy")
    last_x, last_y = lax.axis_size("sx") - 1, lax.axis_size("sy") - 1
    odd_x = ix % 2
    wx, rows = 2 * hx, 2 * hy * cin
    lip = RIM * cin
    near_at = jnp.where(odd_x == 1, 0, RIM + wx)
    far_at = RIM + wx - near_at
    vf[RIM : RIM + wx, lip : lip + rows, :] = block_ref[...].astype(F32)
    vf[pl.ds(near_at, RIM), lip : lip + rows, :] = near_ref[:, 0:rows].astype(F32)
    vf[pl.ds(far_at, RIM), lip : lip + rows, :] = far_ref[:, 0:rows].astype(F32)
    for at, count, piece in (
        (RIM, wx, side_ref[...]),
        (near_at, RIM, near_ref[:, rows : rows + lip]),
        (far_at, RIM, far_ref[:, rows : rows + lip]),
    ):
        piece = piece.astype(F32)
        vf[pl.ds(at, count), 0:lip, :] = jnp.where(iy == 0, 0.0, piece)
        vf[pl.ds(at, count), lip + rows : 2 * lip + rows, :] = jnp.where(iy == 0, piece, 0.0)
    ri = lax.broadcasted_iota(jnp.int32, (2 * lanes, 4 * lanes), 0)
    ci = lax.broadcasted_iota(jnp.int32, (2 * lanes, 4 * lanes), 1)
    sel = one_hot(
        ((ri // lanes) == ((ci % lanes) // hz))
        & ((ri % lanes) == 2 * (ci % hz) + ci // lanes - 1)
    )
    for p in range(pairs):
        for half in range(2):
            cell = 2 * p + half
            cx, cy = cell // ny, cell % ny
            for dx in range(4):
                lhs[
                    p * win + dx * 4 * cin : p * win + (dx + 1) * 4 * cin,
                    half * lanes : (half + 1) * lanes,
                ] = vf[2 * cx + dx, 2 * cin * cy : 2 * cin * cy + 4 * cin, :].astype(BF16)
    picked = mm(lhs[...], sel).astype(BF16)
    for p in range(pairs):
        for o in range(4):
            s_ref[o * win : (o + 1) * win, p * lanes : (p + 1) * lanes] = picked[
                p * win : (p + 1) * win, o * lanes : (o + 1) * lanes
            ]

    wide = w1_ref.shape[1]
    fi = lax.broadcasted_iota(jnp.int32, (4 * win, wide), 0)
    ni = lax.broadcasted_iota(jnp.int32, (4 * win, wide), 1)
    k = ni // cin
    base = (k % 3) * win + (k // 9) * 4 * cin + ((k // 3) % 3) * cin + ni % cin
    diff = fi - base
    folds = [
        one_hot(diff == fz * win + fx * 4 * cin + fy * cin)
        for fx in range(2)
        for fy in range(2)
        for fz in range(2)
    ]
    w1 = w1_ref[...]
    toeplitz = jnp.concatenate([mm(w1, f, NT).astype(BF16) for f in folds], axis=0)

    lane = lax.broadcasted_iota(jnp.int32, (1, row), 1)
    low_y = jnp.where(iy == 0, hz, 0)
    high_y = jnp.where(iy == last_y, row - hz, row)
    mask_y = jnp.where((lane >= low_y) & (lane < high_y), 1.0, 0.0).astype(F32)
    not_first = jnp.where(lane % hz == 0, 0.0, 1.0).astype(F32)
    not_last = jnp.where(lane % hz == hz - 1, 0.0, 1.0).astype(F32)

    own = hy * hz
    for cx in range(nx):
        here = slice(cx * row, (cx + 1) * row)
        pre = mm(toeplitz, s_ref[:, here])
        t = jnp.exp(-jnp.abs(pre))
        r = 1.0 / (1.0 + t)
        soft = jnp.maximum(pre, 0.0) + jnp.log(1.0 + t)
        sig = jnp.where(pre >= 0, r, t * r)
        hidden = (0.3 * pre + 0.7 * soft).astype(BF16).astype(F32)
        mask = mask_y
        if cx == 0:
            mask = mask * jnp.where(ix == 0, 0.0, 1.0)
        if cx == nx - 1:
            mask = mask * jnp.where(ix == last_x, 0.0, 1.0)
        slope_ref[:, here] = (0.3 + 0.7 * sig) * (mask * 0.125)
        total = hidden[0:c1]
        for s in range(1, 8):
            total = total + hidden[s * c1 : (s + 1) * c1]
        pooled = total * (mask * 0.125)
        three = jnp.concatenate(
            [
                pltpu.roll(pooled, 1, 1) * not_first,
                pooled,
                pltpu.roll(pooled, row - 1, 1) * not_last,
            ],
            axis=0,
        )
        odd = pltpu.roll(three, row - hz, 1).astype(BF16)
        even = three.astype(BF16)
        for a in range(3):
            x = cx - a
            if 0 <= x < hx:
                for b in range(3):
                    at = 3 * c1 * (3 * a + b)
                    piece = odd[:, 0:own] if b == 1 else even[:, b * hz : b * hz + own]
                    cols[at : at + 3 * c1, x * own : (x + 1) * own] = piece

    w2 = w2_ref[...]
    pre2 = mm(w2, cols[...])
    t = jnp.exp(-jnp.abs(pre2))
    r = 1.0 / (1.0 + t)
    slope2 = 0.3 + 0.7 * jnp.where(pre2 >= 0, r, t * r)
    back = (cot_ref[...].astype(F32) * slope2).astype(BF16)
    spread = mm(w2, back, TN)
    second = mm(back, cols[...], NT) * scale_second
    tall = second.shape[1]
    half = second.shape[0] // 2
    is_odd = odd_x == 1
    keep_ref[...] = jnp.zeros(keep_ref.shape, keep_ref.dtype)
    send_ref[...] = jnp.zeros(send_ref.shape, send_ref.dtype)
    keep_ref[:, 0:tall] = jnp.where(is_odd, second[half:], second[:half])
    send_ref[:, 0:tall] = jnp.where(is_odd, second[:half], second[half:]).astype(BF16)

    for cx in range(nx):
        here = slice(cx * row, (cx + 1) * row)
        blocks = []
        for b in range(3):
            acc = None
            for a in range(3):
                x = cx - a
                if 0 <= x < hx:
                    at = 3 * c1 * (3 * a + b)
                    piece = spread[at : at + 3 * c1, x * own : (x + 1) * own]
                    acc = piece if acc is None else acc + piece
            blocks.append(acc)
        gap = jnp.zeros((3 * c1, 2 * hz), F32)
        grown = (
            jnp.concatenate([blocks[0], gap], axis=1)
            + jnp.concatenate([gap, blocks[2]], axis=1)
            + pltpu.roll(jnp.concatenate([blocks[1], gap], axis=1), hz, 1)
        )
        up = (
            pltpu.roll(grown[0:c1], row - 1, 1) * not_last
            + grown[c1 : 2 * c1]
            + pltpu.roll(grown[2 * c1 : 3 * c1], 1, 1) * not_first
        )
        for s in range(8):
            lower[s * c1 : (s + 1) * c1, here] = (
                up * slope_ref[s * c1 : (s + 1) * c1, here]
            ).astype(BF16)

    products = mm(lower[...], s_ref[...], NT)
    high = products.astype(BF16)
    low = (products - high.astype(F32)).astype(BF16)
    first = jnp.zeros((c1, wide), F32)
    for s in range(8):
        part = slice(s * c1, (s + 1) * c1)
        first = first + mm(high[part], folds[s]) + mm(low[part], folds[s])
    first = first * scale_first
    keep_ref[0:c1, g_lane : g_lane + wide] = jnp.where(is_odd, 0.0, first)
    send_ref[0:c1, g_lane : g_lane + wide] = jnp.where(is_odd, first, 0.0).astype(BF16)


def join_kernel(mine_ref, other_ref, first_ref, second_ref, *, g_lane):
    is_odd = lax.axis_index("sx") % 2 == 1
    mine, other = mine_ref[...].astype(F32), other_ref[...].astype(F32)
    upper = jnp.where(is_odd, other, mine)
    half = mine.shape[0]
    tall = second_ref.shape[1]
    c1, wide = first_ref.shape
    second_ref[0:half, :] = upper[:, 0:tall]
    second_ref[half:, :] = jnp.where(is_odd, mine, other)[:, 0:tall]
    first_ref[...] = upper[0:c1, g_lane : g_lane + wide]


def swap(value, axes, mask):
    count = lax.axis_size(axes)
    return lax.ppermute(value, axes, [(i, i ^ mask) for i in range(count)])


def total_over(value, axes, masks):
    for at in range(0, len(masks), 2):
        pair = masks[at : at + 2]
        if len(pair) == 1:
            value = (value.astype(F32) + swap(value, axes, pair[0]).astype(F32)).astype(BF16)
            continue
        m, n = pair
        one, two, three = (swap(value, axes, x).astype(F32) for x in (m, n, m ^ n))
        value = ((value.astype(F32) + one) + (two + three)).astype(BF16)
    return value


def near_core(value):
    return pltpu.with_memory_space_constraint(value, pltpu.VMEM)


def bits(count):
    return [1 << i for i in range(count.bit_length() - 1)]


def shards(volume, first_weight, second_weight, cotangent):
    samples, cin, wx, wy, wz = volume.shape
    hx, hy, hz = wx // 2, wy // 2, wz // 2
    c1, wide = first_weight.shape
    c2, tall = second_weight.shape
    devices = lax.axis_size("dp") * lax.axis_size("sx") * lax.axis_size("sy")
    coarse = samples * hx * hy * hz * devices
    g_lane = -(-tall // 128) * 128
    width = g_lane + -(-wide // 128) * 128
    nx, ny = hx + 2, hy + 2
    lane = nx * ny * hz
    win = 16 * cin

    count_x, count_y = lax.axis_size("sx"), lax.axis_size("sy")
    assert count_y == 2 and count_x & (count_x - 1) == 0 and 2 * c1 == c2
    odd_x = lax.axis_index("sx") % 2 == 1
    low_y = lax.axis_index("sy") == 0
    lip = RIM * cin
    block = volume[0].transpose(1, 2, 0, 3).reshape(wx, wy * cin, wz)

    side = swap(jnp.where(low_y, block[:, -lip:], block[:, :lip]), "sy", 1)
    both = jnp.concatenate([block, side], axis=1)
    inner = jnp.where(odd_x, both[:RIM], both[-RIM:])
    outer = jnp.where(odd_x, both[-RIM:], both[:RIM])
    pairs = [(i, i + 1) for i in range(1, count_x - 1, 2)]
    far = lax.ppermute(outer, "sx", pairs + [(j, i) for i, j in pairs])
    near = swap(inner, "sx", 1)
    cot = cotangent[0].reshape(c2, hx * hy * hz)

    body = functools.partial(
        local_kernel, cin=cin, hx=hx, hy=hy, hz=hz, g_lane=g_lane,
        scale_first=1.0 / math.sqrt(coarse * 8), scale_second=1.0 / math.sqrt(coarse),
    )
    keep, send = pl.pallas_call(
        body,
        out_shape=(
            pltpu.VMEM((c2 // 2, width), F32),
            pltpu.VMEM((c2 // 2, width), BF16),
        ),
        scratch_shapes=[
            pltpu.VMEM((wx + 2 * RIM, (wy + 2 * RIM) * cin, wz), F32),
            pltpu.VMEM((nx * ny // 2 * win, 2 * wz), BF16),
            pltpu.VMEM((4 * win, lane), BF16),
            pltpu.VMEM((8 * c1, lane), F32),
            pltpu.VMEM((tall, hx * hy * hz), BF16),
            pltpu.VMEM((8 * c1, lane), BF16),
        ],
        name="local_step",
    )(*map(near_core, (block, near, far, side, first_weight, second_weight, cot)))
    mine = (keep + swap(send, "sx", 1).astype(F32)).astype(BF16)
    mine = total_over(mine, ("sx", "sy"), [1] + [2 * m for m in bits(count_x)[1:]])
    mine = total_over(mine, ("dp",), bits(lax.axis_size("dp")))
    return pl.pallas_call(
        functools.partial(join_kernel, g_lane=g_lane),
        out_shape=(
            jax.ShapeDtypeStruct((c1, wide), F32),
            jax.ShapeDtypeStruct((c2, tall), F32),
        ),
        name="join",
    )(near_core(mine), near_core(swap(mine, "sx", 1)))


def solution(mesh):
    return jax.shard_map(
        shards,
        mesh=mesh,
        in_specs=(P("dp", None, "sx", "sy", None), P(), P(), P("dp", None, "sx", "sy", None)),
        out_specs=(P(), P()),
        check_vma=False,
    )
```

```python
import functools
import math

import jax
import jax.numpy as jnp
from jax import lax
from jax.experimental import pallas as pl
from jax.experimental.pallas import tpu as pltpu
from jax.sharding import PartitionSpec as P

F32 = jnp.float32
BF16 = jnp.bfloat16
NT = (((1,), (1,)), ((), ()))
RIM = 3
TN = (((0,), (0,)), ((), ()))


def mm(a, b, dims=(((1,), (0,)), ((), ()))):
    return lax.dot_general(a, b, dims, preferred_element_type=F32)


def one_hot(cond):
    return jnp.where(cond, 1.0, 0.0).astype(BF16)


def prepare_kernel(w1_ref, toeplitz_ref, sel_ref, fold_ref, *, cin, hz):
    lanes = 2 * hz
    win = 16 * cin
    ri = lax.broadcasted_iota(jnp.int32, (2 * lanes, 4 * lanes), 0)
    ci = lax.broadcasted_iota(jnp.int32, (2 * lanes, 4 * lanes), 1)
    sel_ref[...] = one_hot(
        ((ri // lanes) == ((ci % lanes) // hz))
        & ((ri % lanes) == 2 * (ci % hz) + ci // lanes - 1)
    )
    wide = w1_ref.shape[1]
    fi = lax.broadcasted_iota(jnp.int32, (4 * win, wide), 0)
    ni = lax.broadcasted_iota(jnp.int32, (4 * win, wide), 1)
    k = ni // cin
    base = (k % 3) * win + (k // 9) * 4 * cin + ((k // 3) % 3) * cin + ni % cin
    diff = fi - base
    folds = [
        one_hot(diff == fz * win + fx * 4 * cin + fy * cin)
        for fx in range(2)
        for fy in range(2)
        for fz in range(2)
    ]
    w1 = w1_ref[...]
    c1 = w1.shape[0]
    for s in range(8):
        fold_ref[s] = folds[s]
        toeplitz_ref[s * c1 : (s + 1) * c1, :] = mm(w1, folds[s], NT).astype(BF16)


def local_kernel(
    block_ref, near_ref, far_ref, side_ref, toeplitz_ref, sel_ref, fold_ref, w2_ref, cot_ref, keep_ref, send_ref,
    vf, lhs, s_ref, slope_ref, cols, lower,
    *, cin, hx, hy, hz, g_lane, scale_first, scale_second,
):
    nx, ny = hx + 2, hy + 2
    row = ny * hz
    c1, wide = toeplitz_ref.shape[0] // 8, fold_ref.shape[2]
    win = 16 * cin
    pairs = nx * ny // 2
    lanes = 2 * hz

    ix, iy = lax.axis_index("sx"), lax.axis_index("sy")
    last_x, last_y = lax.axis_size("sx") - 1, lax.axis_size("sy") - 1
    odd_x = ix % 2
    wx, rows = 2 * hx, 2 * hy * cin
    lip = RIM * cin
    near_at = jnp.where(odd_x == 1, 0, RIM + wx)
    far_at = RIM + wx - near_at
    vf[RIM : RIM + wx, lip : lip + rows, :] = block_ref[...].astype(F32)
    vf[pl.ds(near_at, RIM), lip : lip + rows, :] = near_ref[:, 0:rows].astype(F32)
    vf[pl.ds(far_at, RIM), lip : lip + rows, :] = far_ref[:, 0:rows].astype(F32)
    for at, count, piece in (
        (RIM, wx, side_ref[...]),
        (near_at, RIM, near_ref[:, rows : rows + lip]),
        (far_at, RIM, far_ref[:, rows : rows + lip]),
    ):
        piece = piece.astype(F32)
        vf[pl.ds(at, count), 0:lip, :] = jnp.where(iy == 0, 0.0, piece)
        vf[pl.ds(at, count), lip + rows : 2 * lip + rows, :] = jnp.where(iy == 0, piece, 0.0)
    for p in range(pairs):
        for half in range(2):
            cell = 2 * p + half
            cx, cy = cell // ny, cell % ny
            for dx in range(4):
                lhs[
                    p * win + dx * 4 * cin : p * win + (dx + 1) * 4 * cin,
                    half * lanes : (half + 1) * lanes,
                ] = vf[2 * cx + dx, 2 * cin * cy : 2 * cin * cy + 4 * cin, :].astype(BF16)
    picked = mm(lhs[...], sel_ref[...]).astype(BF16)
    for p in range(pairs):
        for o in range(4):
            s_ref[o * win : (o + 1) * win, p * lanes : (p + 1) * lanes] = picked[
                p * win : (p + 1) * win, o * lanes : (o + 1) * lanes
            ]

    lane = lax.broadcasted_iota(jnp.int32, (1, row), 1)
    low_y = jnp.where(iy == 0, hz, 0)
    high_y = jnp.where(iy == last_y, row - hz, row)
    mask_y = jnp.where((lane >= low_y) & (lane < high_y), 1.0, 0.0).astype(F32)
    not_first = jnp.where(lane % hz == 0, 0.0, 1.0).astype(F32)
    not_last = jnp.where(lane % hz == hz - 1, 0.0, 1.0).astype(F32)

    own = hy * hz
    for cx in range(nx):
        here = slice(cx * row, (cx + 1) * row)
        pre = mm(toeplitz_ref[...], s_ref[:, here])
        t = jnp.exp(-jnp.abs(pre))
        r = 1.0 / (1.0 + t)
        soft = jnp.maximum(pre, 0.0) + jnp.log(1.0 + t)
        sig = jnp.where(pre >= 0, r, t * r)
        hidden = (0.3 * pre + 0.7 * soft).astype(BF16).astype(F32)
        mask = mask_y
        if cx == 0:
            mask = mask * jnp.where(ix == 0, 0.0, 1.0)
        if cx == nx - 1:
            mask = mask * jnp.where(ix == last_x, 0.0, 1.0)
        slope_ref[:, here] = (0.3 + 0.7 * sig) * (mask * 0.125)
        total = hidden[0:c1]
        for s in range(1, 8):
            total = total + hidden[s * c1 : (s + 1) * c1]
        pooled = total * (mask * 0.125)
        three = jnp.concatenate(
            [
                pltpu.roll(pooled, 1, 1) * not_first,
                pooled,
                pltpu.roll(pooled, row - 1, 1) * not_last,
            ],
            axis=0,
        )
        odd = pltpu.roll(three, row - hz, 1).astype(BF16)
        even = three.astype(BF16)
        for a in range(3):
            x = cx - a
            if 0 <= x < hx:
                for b in range(3):
                    at = 3 * c1 * (3 * a + b)
                    piece = odd[:, 0:own] if b == 1 else even[:, b * hz : b * hz + own]
                    cols[at : at + 3 * c1, x * own : (x + 1) * own] = piece

    w2 = w2_ref[...]
    pre2 = mm(w2, cols[...])
    t = jnp.exp(-jnp.abs(pre2))
    r = 1.0 / (1.0 + t)
    slope2 = 0.3 + 0.7 * jnp.where(pre2 >= 0, r, t * r)
    back = (cot_ref[...].astype(F32) * slope2).astype(BF16)
    spread = mm(w2, back, TN)
    second = mm(back, cols[...], NT) * scale_second
    tall = second.shape[1]
    half = second.shape[0] // 2
    is_odd = odd_x == 1
    keep_ref[...] = jnp.zeros(keep_ref.shape, keep_ref.dtype)
    send_ref[...] = jnp.zeros(send_ref.shape, send_ref.dtype)
    keep_ref[:, 0:tall] = jnp.where(is_odd, second[half:], second[:half])
    send_ref[:, 0:tall] = jnp.where(is_odd, second[:half], second[half:]).astype(BF16)

    for cx in range(nx):
        here = slice(cx * row, (cx + 1) * row)
        blocks = []
        for b in range(3):
            acc = None
            for a in range(3):
                x = cx - a
                if 0 <= x < hx:
                    at = 3 * c1 * (3 * a + b)
                    piece = spread[at : at + 3 * c1, x * own : (x + 1) * own]
                    acc = piece if acc is None else acc + piece
            blocks.append(acc)
        gap = jnp.zeros((3 * c1, 2 * hz), F32)
        grown = (
            jnp.concatenate([blocks[0], gap], axis=1)
            + jnp.concatenate([gap, blocks[2]], axis=1)
            + pltpu.roll(jnp.concatenate([blocks[1], gap], axis=1), hz, 1)
        )
        up = (
            pltpu.roll(grown[0:c1], row - 1, 1) * not_last
            + grown[c1 : 2 * c1]
            + pltpu.roll(grown[2 * c1 : 3 * c1], 1, 1) * not_first
        )
        for s in range(8):
            lower[s * c1 : (s + 1) * c1, here] = (
                up * slope_ref[s * c1 : (s + 1) * c1, here]
            ).astype(BF16)

    products = mm(lower[...], s_ref[...], NT)
    high = products.astype(BF16)
    low = (products - high.astype(F32)).astype(BF16)
    first = jnp.zeros((c1, wide), F32)
    for s in range(8):
        part = slice(s * c1, (s + 1) * c1)
        first = first + mm(high[part], fold_ref[s]) + mm(low[part], fold_ref[s])
    first = first * scale_first
    keep_ref[0:c1, g_lane : g_lane + wide] = jnp.where(is_odd, 0.0, first)
    send_ref[0:c1, g_lane : g_lane + wide] = jnp.where(is_odd, first, 0.0).astype(BF16)


def join_kernel(mine_ref, other_ref, first_ref, second_ref, *, g_lane):
    is_odd = lax.axis_index("sx") % 2 == 1
    mine, other = mine_ref[...].astype(F32), other_ref[...].astype(F32)
    upper = jnp.where(is_odd, other, mine)
    half = mine.shape[0]
    tall = second_ref.shape[1]
    c1, wide = first_ref.shape
    second_ref[0:half, :] = upper[:, 0:tall]
    second_ref[half:, :] = jnp.where(is_odd, mine, other)[:, 0:tall]
    first_ref[...] = upper[0:c1, g_lane : g_lane + wide]


def swap(value, axes, mask):
    count = lax.axis_size(axes)
    return lax.ppermute(value, axes, [(i, i ^ mask) for i in range(count)])


def total_over(value, axes, masks):
    for at in range(0, len(masks), 2):
        pair = masks[at : at + 2]
        if len(pair) == 1:
            value = (value.astype(F32) + swap(value, axes, pair[0]).astype(F32)).astype(BF16)
            continue
        m, n = pair
        one, two, three = (swap(value, axes, x).astype(F32) for x in (m, n, m ^ n))
        value = ((value.astype(F32) + one) + (two + three)).astype(BF16)
    return value


def near_core(value):
    return pltpu.with_memory_space_constraint(value, pltpu.VMEM)


def bits(count):
    return [1 << i for i in range(count.bit_length() - 1)]


def shards(volume, first_weight, second_weight, cotangent):
    samples, cin, wx, wy, wz = volume.shape
    hx, hy, hz = wx // 2, wy // 2, wz // 2
    c1, wide = first_weight.shape
    c2, tall = second_weight.shape
    devices = lax.axis_size("dp") * lax.axis_size("sx") * lax.axis_size("sy")
    coarse = samples * hx * hy * hz * devices
    g_lane = -(-tall // 128) * 128
    width = g_lane + -(-wide // 128) * 128
    nx, ny = hx + 2, hy + 2
    lane = nx * ny * hz
    win = 16 * cin

    count_x, count_y = lax.axis_size("sx"), lax.axis_size("sy")
    assert count_y == 2 and count_x & (count_x - 1) == 0 and 2 * c1 == c2
    odd_x = lax.axis_index("sx") % 2 == 1
    low_y = lax.axis_index("sy") == 0
    lip = RIM * cin
    block = volume[0].transpose(1, 2, 0, 3).reshape(wx, wy * cin, wz)

    side = swap(jnp.where(low_y, block[:, -lip:], block[:, :lip]), "sy", 1)
    both = jnp.concatenate([block, side], axis=1)
    inner = jnp.where(odd_x, both[:RIM], both[-RIM:])
    outer = jnp.where(odd_x, both[-RIM:], both[:RIM])
    pairs = [(i, i + 1) for i in range(1, count_x - 1, 2)]
    far = lax.ppermute(outer, "sx", pairs + [(j, i) for i, j in pairs])
    near = swap(inner, "sx", 1)
    cot = cotangent[0].reshape(c2, hx * hy * hz)

    toeplitz, sel, folds = pl.pallas_call(
        functools.partial(prepare_kernel, cin=cin, hz=hz),
        out_shape=(
            pltpu.VMEM((8 * c1, 4 * win), BF16),
            pltpu.VMEM((2 * wz, 4 * wz), BF16),
            pltpu.VMEM((8, 4 * win, wide), BF16),
        ),
        cost_estimate=pl.CostEstimate(
            flops=10**8, bytes_accessed=10**6, transcendentals=0
        ),
        name="prepare",
    )(near_core(first_weight))

    body = functools.partial(
        local_kernel, cin=cin, hx=hx, hy=hy, hz=hz, g_lane=g_lane,
        scale_first=1.0 / math.sqrt(coarse * 8), scale_second=1.0 / math.sqrt(coarse),
    )
    keep, send = pl.pallas_call(
        body,
        out_shape=(
            pltpu.VMEM((c2 // 2, width), F32),
            pltpu.VMEM((c2 // 2, width), BF16),
        ),
        scratch_shapes=[
            pltpu.VMEM((wx + 2 * RIM, (wy + 2 * RIM) * cin, wz), F32),
            pltpu.VMEM((nx * ny // 2 * win, 2 * wz), BF16),
            pltpu.VMEM((4 * win, lane), BF16),
            pltpu.VMEM((8 * c1, lane), F32),
            pltpu.VMEM((tall, hx * hy * hz), BF16),
            pltpu.VMEM((8 * c1, lane), BF16),
        ],
        name="local_step",
    )(*map(near_core, (block, near, far, side, toeplitz, sel, folds, second_weight, cot)))
    mine = (keep + swap(send, "sx", 1).astype(F32)).astype(BF16)
    mine = total_over(mine, ("sx", "sy"), [1] + [2 * m for m in bits(count_x)[1:]])
    mine = total_over(mine, ("dp",), bits(lax.axis_size("dp")))
    return pl.pallas_call(
        functools.partial(join_kernel, g_lane=g_lane),
        out_shape=(
            jax.ShapeDtypeStruct((c1, wide), F32),
            jax.ShapeDtypeStruct((c2, tall), F32),
        ),
        name="join",
    )(near_core(mine), near_core(swap(mine, "sx", 1)))


def solution(mesh):
    return jax.shard_map(
        shards,
        mesh=mesh,
        in_specs=(P("dp", None, "sx", "sy", None), P(), P(), P("dp", None, "sx", "sy", None)),
        out_specs=(P(), P()),
        check_vma=False,
    )
```
